32 devices in a mesh: dp: 4 (over x, y), ep: 8 (over z, core).
Axes of the slice: x: 2, y: 2, z: 4, core: 2. Of those that a mesh axis runs over, the one named last changes fastest.
Arguments:
- x: bfloat16 [4, 8, 256, 5120], P('dp', 'ep'), parts along dimension 0
- expert: int32 [4, 8, 256, 6], P('dp', 'ep'), parts along dimension 0
- slot: int32 [4, 8, 256, 6], P('dp', 'ep'), parts along dimension 0
- gate: float32 [4, 8, 256, 6], P('dp', 'ep'), parts along dimension 0
- w_gate: bfloat16 [40, 5120, 1536], P('ep')
- w_up: bfloat16 [40, 5120, 1536], P('ep')
- w_down: bfloat16 [40, 1536, 5120], P('ep')
- s_gate: bfloat16 [5120, 3072], replicated
- s_up: bfloat16 [5120, 3072], replicated
- s_down: bfloat16 [3072, 5120], replicated
Outputs:
- y: bfloat16 [4, 8, 256, 5120], P('dp', 'ep'), parts along dimension 0
There are 4 independent parts. The reference program is written for one: setup_inputs(seed, part) draws one part's arguments, and reference() takes and returns one part's arrays. A program takes and returns all parts, laid end to end along the dimension named above; an argument that names none is the same for every part.
All inputs are finite; a program needn't handle non-finite values.
Results may differ from the reference program's by a relative error of at most 0.009.
Values are sent between devices in bfloat16 or wider.
A program may use at most 2 GiB of HBM per device.

```python
import jax
import jax.numpy as jnp

MEMBERS = 8
TOKENS = 256
D = 5120
FF = 1536
TOP = 6
EXPERTS = 40
SHARED_FF = 3072
SLOTS = 5 * TOKENS * TOP // (4 * EXPERTS)


def setup_inputs(seed: int = 0, part: int = 0) -> dict:
    own, k1, k2, k3, k4, k5, k6 = jax.random.split(jax.random.key(seed), 7)
    kx, ke, kl, kg = jax.random.split(jax.random.fold_in(own, part), 4)
    devices = (1, MEMBERS)
    place = jax.random.permutation(kl, jnp.arange(EXPERTS, dtype=jnp.uint32))
    slow = ((EXPERTS + (9 * place) % EXPERTS) << ((9 * place) // EXPERTS)) // EXPERTS
    wait = (jax.random.bits(ke, (*devices, TOKENS, EXPERTS), jnp.uint32) >> 10) * slow
    expert = jnp.argsort(wait, axis=-1)[..., :TOP].astype(jnp.int32)
    chosen = jax.nn.one_hot(expert, EXPERTS, dtype=jnp.int32)
    in_line = jnp.cumsum(chosen.reshape(*devices, TOKENS * TOP, EXPERTS), axis=2) - 1
    slot = jnp.sum(in_line.reshape(chosen.shape) * chosen, axis=-1)

    def one(key, rows, columns):
        return (jax.random.normal(key, (rows, columns), jnp.float32) * rows**-0.5).astype(jnp.bfloat16)

    def weights(key, rows, columns):
        return jax.lax.map(lambda k: one(k, rows, columns), jax.random.split(key, EXPERTS))

    return {
        "x": jax.random.normal(kx, (*devices, TOKENS, D), jnp.float32).astype(jnp.bfloat16),
        "expert": expert,
        "slot": slot,
        "gate": jax.nn.softmax(jax.random.normal(kg, expert.shape, jnp.float32)),
        "w_gate": weights(k1, D, FF),
        "w_up": weights(k2, D, FF),
        "w_down": weights(k3, FF, D),
        "s_gate": one(k4, D, SHARED_FF),
        "s_up": one(k5, D, SHARED_FF),
        "s_down": one(k6, SHARED_FF, D),
    }


def einsum(form, a, b):
    return jnp.einsum(form, a.astype(jnp.float32), b.astype(jnp.float32))


def for_all(x, s_gate, s_up, s_down):
    h = jax.nn.silu(einsum("...d,df->...f", x, s_gate)) * einsum("...d,df->...f", x, s_up)
    return einsum("...f,fd->...d", h.astype(jnp.bfloat16), s_down)


def reference(x, expert, slot, gate, w_gate, w_up, w_down, s_gate, s_up, s_down):
    to_expert = jax.nn.one_hot(expert, EXPERTS, dtype=jnp.bfloat16)
    to_slot = jax.nn.one_hot(slot, SLOTS, dtype=jnp.bfloat16)
    weighted = to_expert * gate[..., None].astype(jnp.bfloat16)
    dispatch = einsum("abtke,abtkc->abtec", to_expert, to_slot).astype(jnp.bfloat16)
    combine = einsum("abtke,abtkc->abtec", weighted, to_slot).astype(jnp.bfloat16)
    z = einsum("abtec,abtd->aebcd", dispatch, x).astype(jnp.bfloat16)
    h = jax.nn.silu(einsum("aebcd,edf->aebcf", z, w_gate))
    h = (h * einsum("aebcd,edf->aebcf", z, w_up)).astype(jnp.bfloat16)
    out = einsum("aebcf,efd->aebcd", h, w_down).astype(jnp.bfloat16)
    y = einsum("abtec,aebcd->abtd", combine, out)
    return (y + for_all(x, s_gate, s_up, s_down)).astype(jnp.bfloat16)
```

```python
import jax
import jax.numpy as jnp
from jax import lax
from jax.sharding import PartitionSpec as P

F32 = jnp.float32
BF16 = jnp.bfloat16


def dot(form, a, b):
    return jnp.einsum(form, a, b, preferred_element_type=F32)


def solution(mesh):
    members = mesh.shape["ep"]

    def local(x, expert, slot, gate, w_gate, w_up, w_down, s_gate, s_up, s_down):
        own, (tokens, top) = w_gate.shape[0], expert.shape[2:]
        experts = own * members
        slots = 5 * tokens * top // (4 * experts)
        rows = own * slots
        x = x[0, 0]
        me = lax.axis_index("ep")
        place = jnp.where(slot[0, 0] < slots, expert[0, 0] * slots + slot[0, 0], -1)
        place = lax.all_gather(place, "ep") - me * rows
        gates = lax.all_gather(gate[0, 0], "ep").astype(BF16)
        hit = place[..., None] == lax.broadcasted_iota(jnp.int32, (1, 1, 1, rows), 3)
        dispatch = jnp.any(hit, axis=2).astype(BF16)
        combine = jnp.sum(jnp.where(hit, gates[..., None].astype(F32), 0.0), axis=2).astype(BF16)

        everyone = lax.all_gather(x, "ep")
        a = jax.nn.silu(dot("td,df->tf", x, s_gate)) * dot("td,df->tf", x, s_up)
        shared = dot("tf,fd->td", a.astype(BF16), s_down)
        z = dot("btr,btd->brd", dispatch, everyone).astype(BF16)
        z = z.reshape(members, own, slots, -1)
        h = jax.nn.silu(dot("becd,edf->ebcf", z, w_gate)) * dot("becd,edf->ebcf", z, w_up)
        out = dot("ebcf,efd->becd", h.astype(BF16), w_down).astype(BF16)
        out = out.reshape(members, rows, -1)
        y = dot("btr,brd->btd", combine, out).astype(BF16)
        y = lax.psum_scatter(y, "ep", scatter_dimension=0, tiled=False)
        return (y.astype(F32) + shared).astype(BF16)[None, None]

    by_token = P("dp", "ep", None, None)
    by_expert = P("ep", None, None)
    whole = P(None, None)
    return jax.shard_map(
        local,
        mesh=mesh,
        in_specs=(by_token,) * 4 + (by_expert,) * 3 + (whole,) * 3,
        out_specs=by_token,
        check_vma=False,
    )
```

```python
import functools

import jax
import jax.numpy as jnp
from jax import lax
from jax.experimental import pallas as pl
from jax.experimental.pallas import tpu as pltpu
from jax.sharding import PartitionSpec as P

F32 = jnp.float32
BF16 = jnp.bfloat16
W = 256
NL = 6
NT = 6
MESH = pl.DeviceIdType.MESH


def mm(a, b):
    return jnp.dot(a, b, preferred_element_type=F32)


def kernel(
    x, disp, comb, wg, wu, wd, sg, su, sd, y,
    xg, acc, tot, h, sh, gring, dring, zb, ob, pb, dl, rl, ll, csr, csl, yb,
    agr, ags, gsem, dsem, dlr, dls, rrec, lrec, rsend, lsend, ysem, free_r, free_l, free_p,
):
    tokens, depth = x.shape
    own, _, ff = wg.shape
    slots = disp.shape[1] // own
    nq = depth // W
    deep = 2 * W
    me = lax.axis_index("ep")
    z, c = me // 2, me % 2
    left, right, partner = {"ep": me - 2}, {"ep": me + 2}, {"ep": z * 2 + 1 - c}

    def send(src, dst, ssem, rsem, to):
        return pltpu.make_async_remote_copy(
            src_ref=src, dst_ref=dst, send_sem=ssem, recv_sem=rsem, device_id=to, device_id_type=MESH
        )

    def signal(sem, to):
        pl.semaphore_signal(sem, inc=1, device_id=to, device_id_type=MESH)

    shared_tiles = 4 * (depth // deep)
    per_pass = 2 * own * (depth // deep)
    all_tiles = shared_tiles + 2 * per_pass

    def g_copy(src, slot):
        return pltpu.make_async_copy(src, gring.at[slot], gsem.at[slot])

    def g_start(g):
        slot = g % 4

        @pl.when(g < shared_tiles)
        def _():
            rows = pl.ds((g // 4) * deep, deep)
            t = g % 4

            @pl.when(t < 2)
            def _():
                g_copy(sg.at[rows, pl.ds(pl.multiple_of((t % 2) * ff, 128), ff)], slot).start()

            @pl.when(t >= 2)
            def _():
                g_copy(su.at[rows, pl.ds(pl.multiple_of((t % 2) * ff, 128), ff)], slot).start()

        @pl.when((g >= shared_tiles) & (g < all_tiles))
        def _():
            r = (g - shared_tiles) % per_pass
            rows = pl.ds((r // (2 * own)) * deep, deep)
            t = r % (2 * own)

            @pl.when(t < own)
            def _():
                g_copy(wg.at[t % own, rows, :], slot).start()

            @pl.when(t >= own)
            def _():
                g_copy(wu.at[t % own, rows, :], slot).start()

    def g_wait(g):
        g_copy(wg.at[0, pl.ds(0, deep), :], g % 4).wait()

    def d_copy(src, slot):
        return pltpu.make_async_copy(src, dring.at[slot], dsem.at[slot])

    def d_start(g, nt):
        slot = g % 4
        t = g % nt
        cols = pl.ds(pl.multiple_of((g // nt) * W, W), W)

        @pl.when((g < nq * nt) & (t < own))
        def _():
            d_copy(wd.at[t % own, :, cols], slot).start()

        @pl.when((g < nq * nt) & (t >= own))
        def _():
            d_copy(sd.at[pl.ds(((t - own) % 2) * ff, ff), cols], slot).start()

    def d_wait(g):
        d_copy(wd.at[0, :, pl.ds(0, W)], g % 4).wait()

    def hop(q, src, kind, to):
        piece = xg.at[c * nq + q, src]
        return send(piece, piece, ags.at[kind, src, q % 2], agr.at[c * nq + q, src], to)

    def hop_start(q, src, kind, to):
        @pl.when(q >= 2)
        def _():
            hop(q - 2, src, kind, to).wait_send()

        hop(q, src, kind, to).start()

    def spread(clock):
        for src in range(4):
            q = clock - c * nq - jnp.abs(z - src)

            @pl.when((q >= 0) & (q < nq))
            def _():
                @pl.when(z != src)
                def _():
                    hop(q, src, 0, right).wait_recv()

                @pl.when((z >= src) & (z < 3))
                def _():
                    hop_start(q, src, 0, right)

                @pl.when((z <= src) & (z > 0))
                def _():
                    hop_start(q, src, 1, left)

                hop_start(q, src, 2, partner)

    def own_piece(q):
        return pltpu.make_async_copy(
            x.at[:, pl.ds(pl.multiple_of(q * W, W), W)], xg.at[c * nq + q, z], agr.at[c * nq + q, z]
        )

    barrier = pltpu.get_barrier_semaphore()

    @pl.when(z > 0)
    def _():
        signal(barrier, left)

    @pl.when(z < 3)
    def _():
        signal(barrier, right)

    signal(barrier, partner)

    @pl.loop(0, nq)
    def _(q):
        own_piece(q).start()

    for g in range(3):
        g_start(jnp.int32(g))

    @pl.loop(0, 4 * NT)
    def _(b):
        tot[b] = jnp.zeros((tokens, W), F32)

    @pl.loop(0, 2 * own)
    def _(b):
        acc[b] = jnp.zeros((4 * slots, ff), F32)

    @pl.loop(0, nq)
    def _(q):
        own_piece(q).wait()

    pl.semaphore_wait(barrier, 1 + (z > 0).astype(jnp.int32) + (z < 3).astype(jnp.int32))

    @pl.loop(0, depth // deep)
    def _(k):
        @pl.when(k % 2 == 0)
        def _():
            spread(k // 2)

        @pl.loop(0, 4)
        def _(t):
            g = 4 * k + t
            g_start(g + 3)
            g_wait(g)
            a = [xg[c * nq + 2 * k + i, z] for i in range(2)]
            for n in range(ff // W):
                w = gring.at[g % 4, :, pl.ds(n * W, W)]
                tot[t * (ff // W) + n] += mm(a[0], w[:W]) + mm(a[1], w[W:])

    half = 2 * ff // W
    for n in range(half):
        v = tot[n]
        sh[n // (ff // W), :, pl.ds(n % (ff // W) * W, W)] = (jax.nn.silu(v) * tot[half + n]).astype(BF16)

    def up(u):
        s, k, part = u // nq, (u % nq) // 2, u % 2

        @pl.when(part == 0)
        def _():
            @pl.when(c != s)
            def _():
                for i in range(2):
                    for src in range(4):
                        piece = xg.at[s * nq + 2 * k + i, src]
                        send(piece, piece, ags.at[0, src, 0], agr.at[s * nq + 2 * k + i, src], partner).wait_recv()

            @pl.loop(0, 4)
            def _(src):
                for i in range(2):
                    v = mm(disp[2 * src + s], xg[s * nq + 2 * k + i, src]).astype(BF16)
                    for e in range(own):
                        zb[e, src, :, pl.ds(i * W, W)] = v[e * slots : (e + 1) * slots]

        @pl.loop(0, own)
        def _(e):
            g = shared_tiles + u * own + e
            g_start(g + 3)
            g_wait(g)
            a = zb[e].reshape(4 * slots, deep)
            for n in range(ff // 512):
                cols = pl.ds(n * 512, 512)
                acc[part * own + e, :, cols] += mm(a, gring[g % 4, :, cols])

    def middle():
        @pl.loop(0, own)
        def _(e):
            for n in range(ff // 512):
                cols = pl.ds(n * 512, 512)
                h[e, :, cols] = (jax.nn.silu(acc[e, :, cols]) * acc[own + e, :, cols]).astype(BF16)
                acc[e, :, cols] = jnp.zeros((4 * slots, 512), F32)
                acc[own + e, :, cols] = jnp.zeros((4 * slots, 512), F32)

    def to_partner(j):
        return send(pb.at[j % 2], dl.at[j % 2], dls.at[j % 2], dlr.at[j % 2], partner)

    def down(clock):
        s, j = clock // nq, clock % nq
        mine = c == s
        nt = own + 2 * mine.astype(jnp.int32)
        base = j * nt
        held = (j % NT) * 4

        @pl.when(j == 0)
        def _():
            for g in range(3):
                d_start(jnp.int32(g), nt)

        @pl.loop(0, own)
        def _(e):
            d_start(base + e + 3, nt)
            d_wait(base + e)
            v = mm(h[e], dring[(base + e) % 4]).astype(BF16)
            for d in range(4):
                ob[d, e] = v[d * slots : (d + 1) * slots]

        @pl.when(mine)
        def _():
            @pl.loop(0, 4)
            def _(d):
                tot[held + d] = mm(comb[2 * d + s], ob[d].reshape(own * slots, W))

            for t in range(2):
                g = base + own + t
                d_start(g + 3, nt)
                d_wait(g)
                tot[held + z] += mm(sh[t], dring[g % 4])

        @pl.when(jnp.logical_not(mine))
        def _():
            @pl.when(j >= 2)
            def _():
                to_partner(j - 2).wait_send()
                pl.semaphore_wait(free_p, 1)

            @pl.loop(0, 4)
            def _(d):
                pb[j % 2, d] = mm(comb[2 * d + s], ob[d].reshape(own * slots, W)).astype(BF16)

            to_partner(j).start()

    def chain_r(j, d):
        return send(csr.at[j % 2, d - 1], rl.at[j % NL, d - 1], rsend.at[j % 2, d], rrec.at[j % NL, d], right)

    def chain_l(j, d):
        return send(csl.at[j % 2, d], ll.at[j % NL, d], lsend.at[j % 2, d], lrec.at[j % NL, d], left)

    def out_copy(j):
        return pltpu.make_async_copy(yb.at[j % 2], y.at[:, pl.ds(pl.multiple_of(j * W, W), W)], ysem.at[j % 2])

    def collect(clock):
        j = clock - c * nq

        def within(v):
            return (v >= 0) & (v < nq)

        jm = j - 1

        @pl.when(within(jm))
        def _():
            to_partner(jm).wait_recv()

            @pl.loop(0, 4)
            def _(d):
                tot[(jm % NT) * 4 + d] += dl[jm % 2, d].astype(F32)

            @pl.when(jm < nq - 2)
            def _():
                signal(free_p, partner)

        def pass_on(jr, d, first, chain, buf, land, free, to, back):
            @pl.when(jr >= 2)
            def _():
                chain(jr - 2, d).wait_send()

            @pl.when(jr >= NL)
            def _():
                pl.semaphore_wait(free.at[d], 1)

            b = (jr % NT) * 4 + d

            @pl.when(first)
            def _():
                buf[jr % 2] = tot[b].astype(BF16)

            @pl.when(jnp.logical_not(first))
            def _():
                chain(jr, d).wait_recv()
                buf[jr % 2] = (tot[b] + land[jr % NL].astype(F32)).astype(BF16)

                @pl.when(jr < nq - NL)
                def _():
                    signal(free.at[d], back)

            chain(jr, d).start()

        jr = j - 1 - z
        for d in (3, 2, 1):

            @pl.when(within(jr) & (z < d))
            def _():
                pass_on(jr, d, z == 0, chain_r, csr.at[:, d - 1], rl.at[:, d - 1], free_r, right, left)

        jl = j - 1 - (3 - z)
        for d in (0, 1, 2):

            @pl.when(within(jl) & (z > d))
            def _():
                pass_on(jl, d, z == 3, chain_l, csl.at[:, d], ll.at[:, d], free_l, left, right)

        jf = j - 2 - jnp.maximum(z, 3 - z)

        @pl.when(within(jf))
        def _():
            b = (jf % NT) * 4 + z

            @pl.when(z > 0)
            def _():
                chain_r(jf, z).wait_recv()
                tot[b] += rl[jf % NL, z - 1].astype(F32)

                @pl.when(jf < nq - NL)
                def _():
                    signal(free_r.at[z], left)

            @pl.when(z < 3)
            def _():
                chain_l(jf, z).wait_recv()
                tot[b] += ll[jf % NL, z].astype(F32)

                @pl.when(jf < nq - NL)
                def _():
                    signal(free_l.at[z], right)

            @pl.when(jf >= 2)
            def _():
                out_copy(jf - 2).wait()

            yb[jf % 2] = tot[b].astype(BF16)
            out_copy(jf).start()

    @pl.loop(0, 3 * nq + 5)
    def _(u):
        @pl.when(u < 2 * nq)
        def _():
            spread(u + 5)
            up(u)

        @pl.when((u >= nq) & (u < 3 * nq))
        def _():
            down(u - nq)

        @pl.when(u >= nq)
        def _():
            collect(u - nq)

        @pl.when((u == nq - 1) | (u == 2 * nq - 1))
        def _():
            middle()

    for q in (nq - 2, nq - 1):
        for src in range(4):

            @pl.when((z >= src) & (z < 3))
            def _():
                hop(q, src, 0, right).wait_send()

            @pl.when((z <= src) & (z > 0))
            def _():
                hop(q, src, 1, left).wait_send()

            hop(q, src, 2, partner).wait_send()
        for d in range(1, 4):

            @pl.when(z < d)
            def _():
                chain_r(q, d).wait_send()

        for d in range(3):

            @pl.when(z > d)
            def _():
                chain_l(q, d).wait_send()

        to_partner(q).wait_send()
        out_copy(q).wait()


def moe(x, disp, comb, wg, wu, wd, sg, su, sd):
    tokens, depth = x.shape
    own, _, ff = wg.shape
    rows = disp.shape[1]
    slots = rows // own
    nq = depth // W
    dma, regular = pltpu.SemaphoreType.DMA, pltpu.SemaphoreType.REGULAR
    hbm, vmem = pl.BlockSpec(memory_space=pl.ANY), pl.BlockSpec(memory_space=pltpu.VMEM)
    return pl.pallas_call(
        kernel,
        out_shape=jax.ShapeDtypeStruct((tokens, depth), BF16),
        in_specs=[hbm, vmem, vmem] + [hbm] * 6,
        out_specs=hbm,
        scratch_shapes=[
            pltpu.VMEM((2 * nq, 4, tokens, W), BF16),
            pltpu.VMEM((2 * own, 4 * slots, ff), F32),
            pltpu.VMEM((4 * NT, tokens, W), F32),
            pltpu.VMEM((own, 4 * slots, ff), BF16),
            pltpu.VMEM((2, tokens, ff), BF16),
            pltpu.VMEM((4, 2 * W, ff), BF16),
            pltpu.VMEM((4, ff, W), BF16),
            pltpu.VMEM((own, 4, slots, 2 * W), BF16),
            pltpu.VMEM((4, own, slots, W), BF16),
            pltpu.VMEM((2, 4, tokens, W), BF16),
            pltpu.VMEM((2, 4, tokens, W), BF16),
            pltpu.VMEM((NL, 3, tokens, W), BF16),
            pltpu.VMEM((NL, 3, tokens, W), BF16),
            pltpu.VMEM((2, 3, tokens, W), BF16),
            pltpu.VMEM((2, 3, tokens, W), BF16),
            pltpu.VMEM((2, tokens, W), BF16),
            dma((2 * nq, 4)),
            dma((3, 4, 2)),
            dma((4,)),
            dma((4,)),
            dma((2,)),
            dma((2,)),
            dma((NL, 4)),
            dma((NL, 4)),
            dma((2, 4)),
            dma((2, 4)),
            dma((2,)),
            regular((4,)),
            regular((4,)),
            regular,
        ],
        compiler_params=pltpu.CompilerParams(
            collective_id=0, has_side_effects=True, vmem_limit_bytes=67_043_328
        ),
    )(x, disp, comb, wg, wu, wd, sg, su, sd)


def solution(mesh):
    members = mesh.shape["ep"]

    def local(x, expert, slot, gate, w_gate, w_up, w_down, s_gate, s_up, s_down):
        own, (tokens, top) = w_gate.shape[0], expert.shape[2:]
        experts = own * members
        slots = 5 * tokens * top // (4 * experts)
        rows = own * slots
        me = lax.axis_index("ep")
        place = jnp.where(slot[0, 0] < slots, expert[0, 0] * slots + slot[0, 0], -1)
        place = lax.all_gather(place, "ep") - me * rows
        gates = lax.all_gather(gate[0, 0], "ep").astype(BF16)
        hit = place[..., None] == lax.broadcasted_iota(jnp.int32, (1, 1, 1, rows), 3)
        dispatch = jnp.any(hit, axis=2).astype(BF16).transpose(0, 2, 1)
        combine = jnp.sum(jnp.where(hit, gates[..., None].astype(F32), 0.0), axis=2).astype(BF16)
        y = moe(x[0, 0], dispatch, combine, w_gate, w_up, w_down, s_gate, s_up, s_down)
        return y[None, None]

    by_token = P("dp", "ep", None, None)
    by_expert = P("ep", None, None)
    whole = P(None, None)
    return jax.shard_map(
        local,
        mesh=mesh,
        in_specs=(by_token,) * 4 + (by_expert,) * 3 + (whole,) * 3,
        out_specs=by_token,
        check_vma=False,
    )
```

```python
import functools

import jax
import jax.numpy as jnp
from jax import lax
from jax.experimental import pallas as pl
from jax.experimental.pallas import tpu as pltpu
from jax.sharding import PartitionSpec as P

F32 = jnp.float32
BF16 = jnp.bfloat16
W = 256
NL = 4
NT = 6
MESH = pl.DeviceIdType.MESH


def mm(a, b):
    return jnp.dot(a, b, preferred_element_type=F32)


def kernel(
    top, slots,
    x, place, gate, wg, wu, wd, sg, su, sd, y,
    places, gates, disp, comb, xg, acc, tot, h, sh, gring, dring, sring, zb, ob, pb, dl, rl, ll, csr, csl, yb,
    pr, ps, gr, gs, agr, ags, gsem, dsem, ssem, dlr, dls, rrec, lrec, rsend, lsend, ysem, free_r, free_l, free_p,
):
    tokens, depth = x.shape
    own, _, ff = wg.shape
    nq = depth // W
    deep = 2 * W
    me = lax.axis_index("ep")
    z, c = me // 2, me % 2
    left, right, partner = {"ep": me - 2}, {"ep": me + 2}, {"ep": z * 2 + 1 - c}

    def send(src, dst, ssem, rsem, to):
        return pltpu.make_async_remote_copy(
            src_ref=src, dst_ref=dst, send_sem=ssem, recv_sem=rsem, device_id=to, device_id_type=MESH
        )

    def signal(sem, to):
        pl.semaphore_signal(sem, inc=1, device_id=to, device_id_type=MESH)

    ahead = 3
    nk = depth // deep
    routed_base = 4 * nk

    def g_copy(src, g):
        return pltpu.make_async_copy(src, gring.at[g % 4], gsem.at[g % 4])

    def shared_tile(t, k):
        return (sg, su)[t // 2].at[pl.ds(k * deep, deep), pl.ds((t % 2) * ff, ff)]

    def routed_tile(t, k):
        return (wg, wu)[t % 2].at[t // 2, pl.ds(k * deep, deep), :]

    def g_wait(g):
        g_copy(wg.at[0, pl.ds(0, deep), :], g).wait()

    def piece_cols(j):
        return pl.ds(pl.multiple_of(j * W, W), W)

    def d_copy(e, j, g):
        return pltpu.make_async_copy(wd.at[e, :, piece_cols(j)], dring.at[g % 4], dsem.at[g % 4])

    def s_copy(t, j):
        return pltpu.make_async_copy(sd.at[pl.ds(t * ff, ff), piece_cols(j)], sring.at[t], ssem.at[t])

    def hop(q, src, kind, to):
        piece = xg.at[c * nq + q, src]
        return send(piece, piece, ags.at[kind, src, q % 2], agr.at[c * nq + q, src], to)

    def hop_start(q, src, kind, to):
        @pl.when(q >= 2)
        def _():
            hop(q - 2, src, kind, to).wait_send()

        hop(q, src, kind, to).start()

    def leave(q):
        @pl.when((q >= 0) & (q < nq))
        def _():
            @pl.when(z < 3)
            def _():
                hop_start(q, z, 0, right)

            @pl.when(z > 0)
            def _():
                hop_start(q, z, 1, left)

            hop_start(q, z, 2, partner)

    def spread(clock):
        for src in (0, 3, 1, 2):
            q = clock - c * nq - jnp.abs(z - src)

            @pl.when((q >= 0) & (q < nq) & (z != src))
            def _():
                hop(q, src, 0, right).wait_recv()

                @pl.when((z > src) & (z < 3))
                def _():
                    hop_start(q, src, 0, right)

                @pl.when((z < src) & (z > 0))
                def _():
                    hop_start(q, src, 1, left)

                hop_start(q, src, 2, partner)

        leave(clock - c * nq + 1)

    def own_piece(q):
        return pltpu.make_async_copy(
            x.at[:, pl.ds(pl.multiple_of(q * W, W), W)], xg.at[c * nq + q, z], agr.at[c * nq + q, z]
        )

    others = 2 * 4 - 1

    def place_to(o, src, to):
        return send(place, places.at[src], ps.at[o], pr.at[src], to)

    def gate_to(o, src, to):
        return send(gate, gates.at[src], gs.at[o], gr.at[src], to)

    barrier = pltpu.get_barrier_semaphore()
    for o in range(others):
        signal(barrier, {"ep": (me + o + 1) % (others + 1)})

    @pl.loop(0, nq)
    def _(q):
        own_piece(q).start()

    for g in range(ahead):
        g_copy(shared_tile(g, 0), g).start()
    for t in range(2):
        s_copy(t, 0).start()

    @pl.loop(0, 4 * NT)
    def _(b):
        tot[b] = jnp.zeros((tokens, W), F32)

    @pl.loop(0, 2 * own)
    def _(b):
        acc[b] = jnp.zeros((4 * slots, ff), F32)

    @pl.loop(0, nq)
    def _(q):
        own_piece(q).wait()

    pl.semaphore_wait(barrier, others)
    leave(-c * nq)
    for o in range(others):
        to = {"ep": (me + o + 1) % (others + 1)}
        place_to(o, me, to).start()
        gate_to(o, me, to).start()
    places[me] = place[...]
    gates[me] = gate[...]

    def first_half(k, last):
        a = [xg[c * nq + 2 * k + i, z] for i in range(2)]
        for t in range(4):
            g, later = 4 * k + t, t + ahead
            if later < 4:
                tile = shared_tile(later, k)
            else:
                tile = routed_tile(later - 4, 0) if last else shared_tile(later - 4, k + 1)
            g_copy(tile, g + ahead).start()
            g_wait(g)
            for n in range(ff // W):
                w = gring.at[g % 4, :, pl.ds(n * W, W)]
                tot[t * (ff // W) + n] += mm(a[0], w[:W]) + mm(a[1], w[W:])

    @pl.loop(0, nk - 1)
    def _(k):
        @pl.when(k % 3 != 2)
        def _():
            spread(k // 3 * 2 + k % 3)

        first_half(k, False)

    early = (nk - 1) // 3 * 2
    spread(jnp.int32(early))
    first_half(nk - 1, True)

    for o in range(others):
        src = (me + o + 1) % (others + 1)
        place_to(o, src, partner).wait()
        gate_to(o, src, partner).wait()

    rows = own * slots

    @pl.loop(0, others + 1)
    def _(src):
        at = places[src] - me * rows
        at = jnp.where((at >= 0) & (at < rows), at, -1)
        weight = gates[src]
        row = lax.broadcasted_iota(jnp.int32, (tokens, tokens), 0)
        one = jnp.zeros((tokens, tokens), F32)
        weighted = jnp.zeros((tokens, tokens), F32)
        for k in range(top):
            hit = row == at[k : k + 1]
            one = jnp.where(hit, 1.0, one)
            weighted = jnp.where(hit, weight[k : k + 1], weighted)
        disp[src] = one[:rows].astype(BF16)
        comb[src] = weighted.T[:, :rows].astype(BF16)

    half = 2 * ff // W
    for n in range(half):
        v = tot[n]
        sh[n // (ff // W), :, pl.ds(n % (ff // W) * W, W)] = (jax.nn.silu(v) * tot[half + n]).astype(BF16)

    def up(u):
        s, k, part = u // nq, (u % nq) // 2, u % 2

        @pl.when(part == 0)
        def _():
            @pl.when(c != s)
            def _():
                for i in range(2):
                    for src in range(4):
                        piece = xg.at[s * nq + 2 * k + i, src]
                        send(piece, piece, ags.at[0, src, 0], agr.at[s * nq + 2 * k + i, src], partner).wait_recv()

        for half in range(2):

            @pl.when(part == half)
            def _():
                if half == 0:
                    for src in range(4):
                        for i in range(2):
                            v = mm(disp[2 * src + s], xg[s * nq + 2 * k + i, src]).astype(BF16)
                            for e in range(own):
                                zb[e, src, :, pl.ds(i * W, W)] = v[e * slots : (e + 1) * slots]
                for i in range(own):
                    t, g = half * own + i, routed_base + u * own + i
                    later = t + ahead
                    tile = routed_tile(later % (2 * own), k if later < 2 * own else (k + 1) % nk)
                    g_copy(tile, g + ahead).start()
                    g_wait(g)
                    a = zb[t // 2].reshape(4 * slots, deep)
                    for n in range(ff // 512):
                        cols = pl.ds(n * 512, 512)
                        acc[t % 2 * own + t // 2, :, cols] += mm(a, gring[g % 4, :, cols])

    def middle():
        @pl.loop(0, own)
        def _(e):
            for n in range(ff // 512):
                cols = pl.ds(n * 512, 512)
                h[e, :, cols] = (jax.nn.silu(acc[e, :, cols]) * acc[own + e, :, cols]).astype(BF16)
                acc[e, :, cols] = jnp.zeros((4 * slots, 512), F32)
                acc[own + e, :, cols] = jnp.zeros((4 * slots, 512), F32)

    def to_partner(j):
        return send(pb.at[j % 2], dl.at[j % 2], dls.at[j % 2], dlr.at[j % 2], partner)

    def down(clock):
        s, j = clock // nq, clock % nq
        mine = c == s
        base = j * own
        held = (j % NT) * 4

        @pl.when(j == 0)
        def _():
            for g in range(ahead):
                d_copy(g, 0, g).start()

        for e in range(own):
            later = e + ahead
            d_copy(later % own, j if later < own else jnp.minimum(j + 1, nq - 1), base + later).start()
            d_copy(0, 0, base + e).wait()
            v = mm(h[e], dring[(base + e) % 4]).astype(BF16)
            for d in range(4):
                ob[d, e] = v[d * slots : (d + 1) * slots]

        @pl.when(j == nq - 1)
        def _():
            for i in range(ahead):
                d_copy(0, 0, base + own + i).wait()

        @pl.when(mine)
        def _():
            for d in range(4):
                tot[held + d] = mm(comb[2 * d + s], ob[d].reshape(own * slots, W))
            for t in range(2):
                s_copy(t, 0).wait()
            tot[held + z] += mm(sh[0], sring[0]) + mm(sh[1], sring[1])

            @pl.when(j < nq - 1)
            def _():
                for t in range(2):
                    s_copy(t, j + 1).start()

        @pl.when(jnp.logical_not(mine))
        def _():
            @pl.when(j >= 2)
            def _():
                to_partner(j - 2).wait_send()
                pl.semaphore_wait(free_p, 1)

            for d in range(4):
                pb[j % 2, d] = mm(comb[2 * d + s], ob[d].reshape(own * slots, W)).astype(BF16)
            to_partner(j).start()

    def chain_r(j, d):
        return send(csr.at[j % 2, d - 1], rl.at[j % NL, d - 1], rsend.at[j % 2, d], rrec.at[j % NL, d], right)

    def chain_l(j, d):
        return send(csl.at[j % 2, d], ll.at[j % NL, d], lsend.at[j % 2, d], lrec.at[j % NL, d], left)

    def out_copy(j):
        return pltpu.make_async_copy(yb.at[j % 2], y.at[:, pl.ds(pl.multiple_of(j * W, W), W)], ysem.at[j % 2])

    def collect(clock):
        j = clock - c * nq

        def within(v):
            return (v >= 0) & (v < nq)

        jm = j - 1

        @pl.when(within(jm))
        def _():
            to_partner(jm).wait_recv()

            @pl.loop(0, 4)
            def _(d):
                tot[(jm % NT) * 4 + d] += dl[jm % 2, d].astype(F32)

            @pl.when(jm < nq - 2)
            def _():
                signal(free_p, partner)

        def pass_on(jr, d, first, chain, buf, land, free, to, back):
            @pl.when(jr >= 2)
            def _():
                chain(jr - 2, d).wait_send()

            @pl.when(jr >= NL)
            def _():
                pl.semaphore_wait(free.at[d], 1)

            b = (jr % NT) * 4 + d

            @pl.when(first)
            def _():
                buf[jr % 2] = tot[b].astype(BF16)

            @pl.when(jnp.logical_not(first))
            def _():
                chain(jr, d).wait_recv()
                buf[jr % 2] = (tot[b] + land[jr % NL].astype(F32)).astype(BF16)

                @pl.when(jr < nq - NL)
                def _():
                    signal(free.at[d], back)

            chain(jr, d).start()

        jr = j - 1 - z
        for d in (3, 2, 1):

            @pl.when(within(jr) & (z < d))
            def _():
                pass_on(jr, d, z == 0, chain_r, csr.at[:, d - 1], rl.at[:, d - 1], free_r, right, left)

        jl = j - 1 - (3 - z)
        for d in (0, 1, 2):

            @pl.when(within(jl) & (z > d))
            def _():
                pass_on(jl, d, z == 3, chain_l, csl.at[:, d], ll.at[:, d], free_l, left, right)

        jf = j - 2 - jnp.maximum(z, 3 - z)

        @pl.when(within(jf))
        def _():
            b = (jf % NT) * 4 + z

            @pl.when(z > 0)
            def _():
                chain_r(jf, z).wait_recv()
                tot[b] += rl[jf % NL, z - 1].astype(F32)

                @pl.when(jf < nq - NL)
                def _():
                    signal(free_r.at[z], left)

            @pl.when(z < 3)
            def _():
                chain_l(jf, z).wait_recv()
                tot[b] += ll[jf % NL, z].astype(F32)

                @pl.when(jf < nq - NL)
                def _():
                    signal(free_l.at[z], right)

            @pl.when(jf >= 2)
            def _():
                out_copy(jf - 2).wait()

            yb[jf % 2] = tot[b].astype(BF16)
            out_copy(jf).start()

    @pl.loop(0, 3 * nq + 5)
    def _(u):
        @pl.when(u < 2 * nq)
        def _():
            spread(u + early + 1)
            up(u)

        @pl.when((u >= nq) & (u < 3 * nq))
        def _():
            down(u - nq)

        @pl.when(u >= nq)
        def _():
            collect(u - nq)

        @pl.when((u == nq - 1) | (u == 2 * nq - 1))
        def _():
            middle()

    for i in range(ahead):
        g_wait(routed_base + 2 * nq * own + i)
    for q in (nq - 2, nq - 1):
        for src in range(4):

            @pl.when((z >= src) & (z < 3))
            def _():
                hop(q, src, 0, right).wait_send()

            @pl.when((z <= src) & (z > 0))
            def _():
                hop(q, src, 1, left).wait_send()

            hop(q, src, 2, partner).wait_send()
        for d in range(1, 4):

            @pl.when(z < d)
            def _():
                chain_r(q, d).wait_send()

        for d in range(3):

            @pl.when(z > d)
            def _():
                chain_l(q, d).wait_send()

        to_partner(q).wait_send()
        out_copy(q).wait()


def moe(x, place, gate, top, slots, wg, wu, wd, sg, su, sd):
    tokens, depth = x.shape
    own, _, ff = wg.shape
    rows = own * slots
    padded = place.shape[0]
    nq = depth // W
    dma, regular = pltpu.SemaphoreType.DMA, pltpu.SemaphoreType.REGULAR
    hbm, vmem = pl.BlockSpec(memory_space=pl.ANY), pl.BlockSpec(memory_space=pltpu.VMEM)
    return pl.pallas_call(
        functools.partial(kernel, top, slots),
        out_shape=jax.ShapeDtypeStruct((tokens, depth), BF16),
        in_specs=[hbm, vmem, vmem] + [hbm] * 6,
        out_specs=hbm,
        scratch_shapes=[
            pltpu.VMEM((8, padded, tokens), jnp.int32),
            pltpu.VMEM((8, padded, tokens), F32),
            pltpu.VMEM((8, rows, tokens), BF16),
            pltpu.VMEM((8, tokens, rows), BF16),
            pltpu.VMEM((2 * nq, 4, tokens, W), BF16),
            pltpu.VMEM((2 * own, 4 * slots, ff), F32),
            pltpu.VMEM((4 * NT, tokens, W), F32),
            pltpu.VMEM((own, 4 * slots, ff), BF16),
            pltpu.VMEM((2, tokens, ff), BF16),
            pltpu.VMEM((4, 2 * W, ff), BF16),
            pltpu.VMEM((4, ff, W), BF16),
            pltpu.VMEM((2, ff, W), BF16),
            pltpu.VMEM((own, 4, slots, 2 * W), BF16),
            pltpu.VMEM((4, own, slots, W), BF16),
            pltpu.VMEM((2, 4, tokens, W), BF16),
            pltpu.VMEM((2, 4, tokens, W), BF16),
            pltpu.VMEM((NL, 3, tokens, W), BF16),
            pltpu.VMEM((NL, 3, tokens, W), BF16),
            pltpu.VMEM((2, 3, tokens, W), BF16),
            pltpu.VMEM((2, 3, tokens, W), BF16),
            pltpu.VMEM((2, tokens, W), BF16),
            dma((8,)),
            dma((7,)),
            dma((8,)),
            dma((7,)),
            dma((2 * nq, 4)),
            dma((3, 4, 2)),
            dma((4,)),
            dma((4,)),
            dma((2,)),
            dma((2,)),
            dma((2,)),
            dma((NL, 4)),
            dma((NL, 4)),
            dma((2, 4)),
            dma((2, 4)),
            dma((2,)),
            regular((4,)),
            regular((4,)),
            regular,
        ],
        compiler_params=pltpu.CompilerParams(
            collective_id=0, has_side_effects=True, vmem_limit_bytes=67_043_328
        ),
    )(x, place, gate, wg, wu, wd, sg, su, sd)


def solution(mesh):
    members = mesh.shape["ep"]

    def local(x, expert, slot, gate, w_gate, w_up, w_down, s_gate, s_up, s_down):
        own, (tokens, top) = w_gate.shape[0], expert.shape[2:]
        experts = own * members
        slots = 5 * tokens * top // (4 * experts)
        place = jnp.where(slot[0, 0] < slots, expert[0, 0] * slots + slot[0, 0], -1).T
        weight = gate[0, 0].astype(BF16).astype(F32).T
        pad = ((0, -top % 8), (0, 0))
        place, weight = jnp.pad(place, pad, constant_values=-1), jnp.pad(weight, pad)
        y = moe(x[0, 0], place, weight, top, slots, w_gate, w_up, w_down, s_gate, s_up, s_down)
        return y[None, None]

    by_token = P("dp", "ep", None, None)
    by_expert = P("ep", None, None)
    whole = P(None, None)
    return jax.shard_map(
        local,
        mesh=mesh,
        in_specs=(by_token,) * 4 + (by_expert,) * 3 + (whole,) * 3,
        out_specs=by_token,
        check_vma=False,
    )
```

```python
import functools

import jax
import jax.numpy as jnp
from jax import lax
from jax.experimental import pallas as pl
from jax.experimental.pallas import tpu as pltpu
from jax.sharding import PartitionSpec as P

F32 = jnp.float32
BF16 = jnp.bfloat16
W = 256
NL = 4
NT = 6
MESH = pl.DeviceIdType.MESH


def mm(a, b):
    return jnp.dot(a, b, preferred_element_type=F32)


def kernel(
    top, slots,
    x, place, gate, wg, wu, wd, sg, su, sd, y,
    places, gates, disp, comb, xg, acc, tot, h, sh, gring, dring, sring, zb, ob, pb, dl, rl, ll, csr, csl, yb,
    pr, ps, gr, gs, agr, ags, gsem, dsem, ssem, dlr, dls, rrec, lrec, rsend, lsend, ysem, free_r, free_l, free_p,
):
    tokens, depth = x.shape
    own, _, ff = wg.shape
    nq = depth // W
    deep = 2 * W
    me = lax.axis_index("ep")
    z, c = me // 2, me % 2
    left, right, partner = {"ep": me - 2}, {"ep": me + 2}, {"ep": z * 2 + 1 - c}

    def send(src, dst, ssem, rsem, to):
        return pltpu.make_async_remote_copy(
            src_ref=src, dst_ref=dst, send_sem=ssem, recv_sem=rsem, device_id=to, device_id_type=MESH
        )

    def signal(sem, to):
        pl.semaphore_signal(sem, inc=1, device_id=to, device_id_type=MESH)

    ahead = 3
    nk = depth // deep
    routed_base = 4 * nk

    def g_copy(src, g):
        return pltpu.make_async_copy(src, gring.at[g % 4], gsem.at[g % 4])

    def shared_tile(t, k):
        return (sg, su)[t // 2].at[pl.ds(k * deep, deep), pl.ds((t % 2) * ff, ff)]

    def routed_tile(t, k):
        return (wg, wu)[t % 2].at[t // 2, pl.ds(k * deep, deep), :]

    def g_wait(g):
        g_copy(wg.at[0, pl.ds(0, deep), :], g).wait()

    def piece_cols(j):
        return pl.ds(pl.multiple_of(j * W, W), W)

    def d_copy(e, j, g):
        return pltpu.make_async_copy(wd.at[e, :, piece_cols(j)], dring.at[g % 4], dsem.at[g % 4])

    def s_copy(t, j):
        return pltpu.make_async_copy(sd.at[pl.ds(t * ff, ff), piece_cols(j)], sring.at[t], ssem.at[t])

    def hop(q, src, kind, to):
        piece = xg.at[c * nq + q, src]
        return send(piece, piece, ags.at[kind, src, q % 2], agr.at[c * nq + q, src], to)

    def hop_start(q, src, kind, to):
        @pl.when(q >= 2)
        def _():
            hop(q - 2, src, kind, to).wait_send()

        hop(q, src, kind, to).start()

    def leave(q):
        @pl.when((q >= 0) & (q < nq))
        def _():
            @pl.when(z < 3)
            def _():
                hop_start(q, z, 0, right)

            @pl.when(z > 0)
            def _():
                hop_start(q, z, 1, left)

            hop_start(q, z, 2, partner)

    def spread(clock):
        for src in (0, 3, 1, 2):
            q = clock - c * nq - jnp.abs(z - src)

            @pl.when((q >= 0) & (q < nq) & (z != src))
            def _():
                hop(q, src, 0, right).wait_recv()

                @pl.when((z > src) & (z < 3))
                def _():
                    hop_start(q, src, 0, right)

                @pl.when((z < src) & (z > 0))
                def _():
                    hop_start(q, src, 1, left)

                hop_start(q, src, 2, partner)

        leave(clock - c * nq + 1)

    def own_piece(q):
        return pltpu.make_async_copy(
            x.at[:, pl.ds(pl.multiple_of(q * W, W), W)], xg.at[c * nq + q, z], agr.at[c * nq + q, z]
        )

    others = 2 * 4 - 1

    def place_to(o, src, to):
        return send(place, places.at[src], ps.at[o], pr.at[src], to)

    def gate_to(o, src, to):
        return send(gate, gates.at[src], gs.at[o], gr.at[src], to)

    barrier = pltpu.get_barrier_semaphore()
    for o in range(others):
        signal(barrier, {"ep": (me + o + 1) % (others + 1)})

    @pl.loop(0, nq)
    def _(q):
        own_piece(q).start()

    for g in range(ahead):
        g_copy(shared_tile(g, 0), g).start()
    for t in range(2):
        s_copy(t, 0).start()

    @pl.loop(0, 4 * NT)
    def _(b):
        tot[b] = jnp.zeros((tokens, W), F32)

    @pl.loop(0, 2 * own)
    def _(b):
        acc[b] = jnp.zeros((4 * slots, ff), F32)

    @pl.loop(0, nq)
    def _(q):
        own_piece(q).wait()

    pl.semaphore_wait(barrier, others)
    leave(-c * nq)
    for o in range(others):
        to = {"ep": (me + o + 1) % (others + 1)}
        place_to(o, me, to).start()
        gate_to(o, me, to).start()
    places[me] = place[...]
    gates[me] = gate[...]

    def first_half(k, last):
        a = [xg[c * nq + 2 * k + i, z] for i in range(2)]
        for t in range(4):
            g, later = 4 * k + t, t + ahead
            if later < 4:
                tile = shared_tile(later, k)
            else:
                tile = routed_tile(later - 4, 0) if last else shared_tile(later - 4, k + 1)
            g_copy(tile, g + ahead).start()
            g_wait(g)
            for n in range(ff // W):
                w = gring.at[g % 4, :, pl.ds(n * W, W)]
                tot[t * (ff // W) + n] += mm(a[0], w[:W]) + mm(a[1], w[W:])

    @pl.loop(0, nk - 1)
    def _(k):
        @pl.when(k % 2 == 0)
        def _():
            spread(k // 2)

        first_half(k, False)

    first_half(nk - 1, True)
    early = nk // 2
    spread(jnp.int32(early))

    for o in range(others):
        src = (me + o + 1) % (others + 1)
        place_to(o, src, partner).wait()
        gate_to(o, src, partner).wait()

    rows = own * slots

    @pl.loop(0, others + 1)
    def _(src):
        at = places[src] - me * rows
        at = jnp.where((at >= 0) & (at < rows), at, -1)
        weight = gates[src]
        row = lax.broadcasted_iota(jnp.int32, (tokens, tokens), 0)
        one = jnp.zeros((tokens, tokens), F32)
        weighted = jnp.zeros((tokens, tokens), F32)
        for k in range(top):
            hit = row == at[k : k + 1]
            one = jnp.where(hit, 1.0, one)
            weighted = jnp.where(hit, weight[k : k + 1], weighted)
        disp[src] = one[:rows].astype(BF16)
        comb[src] = weighted.T[:, :rows].astype(BF16)

    half = 2 * ff // W
    for n in range(half):
        v = tot[n]
        sh[n // (ff // W), :, pl.ds(n % (ff // W) * W, W)] = (jax.nn.silu(v) * tot[half + n]).astype(BF16)

    def up(u):
        s, k, part = u // nq, (u % nq) // 2, u % 2

        @pl.when(part == 0)
        def _():
            @pl.when(c != s)
            def _():
                for i in range(2):
                    for src in range(4):
                        piece = xg.at[s * nq + 2 * k + i, src]
                        send(piece, piece, ags.at[0, src, 0], agr.at[s * nq + 2 * k + i, src], partner).wait_recv()

        for half in range(2):

            @pl.when(part == half)
            def _():
                if half == 0:
                    for src in range(4):
                        for i in range(2):
                            v = mm(disp[2 * src + s], xg[s * nq + 2 * k + i, src]).astype(BF16)
                            for e in range(own):
                                zb[e, src, :, pl.ds(i * W, W)] = v[e * slots : (e + 1) * slots]
                for i in range(own):
                    t, g = half * own + i, routed_base + u * own + i
                    later = t + ahead
                    tile = routed_tile(later % (2 * own), k if later < 2 * own else (k + 1) % nk)
                    g_copy(tile, g + ahead).start()
                    g_wait(g)
                    a = zb[t // 2].reshape(4 * slots, deep)
                    for n in range(ff // 512):
                        cols = pl.ds(n * 512, 512)
                        acc[t % 2 * own + t // 2, :, cols] += mm(a, gring[g % 4, :, cols])

    def middle():
        @pl.loop(0, own)
        def _(e):
            for n in range(ff // 512):
                cols = pl.ds(n * 512, 512)
                h[e, :, cols] = (jax.nn.silu(acc[e, :, cols]) * acc[own + e, :, cols]).astype(BF16)
                acc[e, :, cols] = jnp.zeros((4 * slots, 512), F32)
                acc[own + e, :, cols] = jnp.zeros((4 * slots, 512), F32)

    def to_partner(j):
        return send(pb.at[j % 2], dl.at[j % 2], dls.at[j % 2], dlr.at[j % 2], partner)

    def down(clock):
        s, j = clock // nq, clock % nq
        mine = c == s
        base = j * own
        held = (j % NT) * 4

        @pl.when(j == 0)
        def _():
            for g in range(ahead):
                d_copy(g, 0, g).start()

        for e in range(own):
            later = e + ahead
            d_copy(later % own, j if later < own else jnp.minimum(j + 1, nq - 1), base + later).start()
            d_copy(0, 0, base + e).wait()
            v = mm(h[e], dring[(base + e) % 4]).astype(BF16)
            for d in range(4):
                ob[d, e] = v[d * slots : (d + 1) * slots]

        @pl.when(j == nq - 1)
        def _():
            for i in range(ahead):
                d_copy(0, 0, base + own + i).wait()

        @pl.when(mine)
        def _():
            for d in range(4):
                tot[held + d] = mm(comb[2 * d + s], ob[d].reshape(own * slots, W))
            for t in range(2):
                s_copy(t, 0).wait()
            tot[held + z] += mm(sh[0], sring[0]) + mm(sh[1], sring[1])

            @pl.when(j < nq - 1)
            def _():
                for t in range(2):
                    s_copy(t, j + 1).start()

        @pl.when(jnp.logical_not(mine))
        def _():
            @pl.when(j >= 2)
            def _():
                to_partner(j - 2).wait_send()
                pl.semaphore_wait(free_p, 1)

            for d in range(4):
                pb[j % 2, d] = mm(comb[2 * d + s], ob[d].reshape(own * slots, W)).astype(BF16)
            to_partner(j).start()

    def chain_r(j, d):
        return send(csr.at[j % 2, d - 1], rl.at[j % NL, d - 1], rsend.at[j % 2, d], rrec.at[j % NL, d], right)

    def chain_l(j, d):
        return send(csl.at[j % 2, d], ll.at[j % NL, d], lsend.at[j % 2, d], lrec.at[j % NL, d], left)

    def out_copy(j):
        return pltpu.make_async_copy(yb.at[j % 2], y.at[:, pl.ds(pl.multiple_of(j * W, W), W)], ysem.at[j % 2])

    def collect(clock):
        j = clock - c * nq

        def within(v):
            return (v >= 0) & (v < nq)

        jm = j - 1

        @pl.when(within(jm))
        def _():
            to_partner(jm).wait_recv()

            @pl.loop(0, 4)
            def _(d):
                tot[(jm % NT) * 4 + d] += dl[jm % 2, d].astype(F32)

            @pl.when(jm < nq - 2)
            def _():
                signal(free_p, partner)

        def pass_on(jr, d, first, chain, buf, land, free, to, back):
            @pl.when(jr >= 2)
            def _():
                chain(jr - 2, d).wait_send()

            @pl.when(jr >= NL)
            def _():
                pl.semaphore_wait(free.at[d], 1)

            b = (jr % NT) * 4 + d

            @pl.when(first)
            def _():
                buf[jr % 2] = tot[b].astype(BF16)

            @pl.when(jnp.logical_not(first))
            def _():
                chain(jr, d).wait_recv()
                buf[jr % 2] = (tot[b] + land[jr % NL].astype(F32)).astype(BF16)

                @pl.when(jr < nq - NL)
                def _():
                    signal(free.at[d], back)

            chain(jr, d).start()

        jr = j - 1 - z
        for d in (3, 2, 1):

            @pl.when(within(jr) & (z < d))
            def _():
                pass_on(jr, d, z == 0, chain_r, csr.at[:, d - 1], rl.at[:, d - 1], free_r, right, left)

        jl = j - 1 - (3 - z)
        for d in (0, 1, 2):

            @pl.when(within(jl) & (z > d))
            def _():
                pass_on(jl, d, z == 3, chain_l, csl.at[:, d], ll.at[:, d], free_l, left, right)

        jf = j - 2 - jnp.maximum(z, 3 - z)

        @pl.when(within(jf))
        def _():
            b = (jf % NT) * 4 + z

            @pl.when(z > 0)
            def _():
                chain_r(jf, z).wait_recv()
                tot[b] += rl[jf % NL, z - 1].astype(F32)

                @pl.when(jf < nq - NL)
                def _():
                    signal(free_r.at[z], left)

            @pl.when(z < 3)
            def _():
                chain_l(jf, z).wait_recv()
                tot[b] += ll[jf % NL, z].astype(F32)

                @pl.when(jf < nq - NL)
                def _():
                    signal(free_l.at[z], right)

            @pl.when(jf >= 2)
            def _():
                out_copy(jf - 2).wait()

            yb[jf % 2] = tot[b].astype(BF16)
            out_copy(jf).start()

    @pl.loop(0, 3 * nq + 5)
    def _(u):
        @pl.when(u < 2 * nq)
        def _():
            @pl.when(u > 0)
            def _():
                spread(u + early)

            up(u)

        @pl.when((u >= nq) & (u < 3 * nq))
        def _():
            down(u - nq)

        @pl.when(u >= nq)
        def _():
            collect(u - nq)

        @pl.when((u == nq - 1) | (u == 2 * nq - 1))
        def _():
            middle()

    for i in range(ahead):
        g_wait(routed_base + 2 * nq * own + i)
    for q in (nq - 2, nq - 1):
        for src in range(4):

            @pl.when((z >= src) & (z < 3))
            def _():
                hop(q, src, 0, right).wait_send()

            @pl.when((z <= src) & (z > 0))
            def _():
                hop(q, src, 1, left).wait_send()

            hop(q, src, 2, partner).wait_send()
        for d in range(1, 4):

            @pl.when(z < d)
            def _():
                chain_r(q, d).wait_send()

        for d in range(3):

            @pl.when(z > d)
            def _():
                chain_l(q, d).wait_send()

        to_partner(q).wait_send()
        out_copy(q).wait()


def moe(x, place, gate, top, slots, wg, wu, wd, sg, su, sd):
    tokens, depth = x.shape
    own, _, ff = wg.shape
    rows = own * slots
    padded = place.shape[0]
    nq = depth // W
    dma, regular = pltpu.SemaphoreType.DMA, pltpu.SemaphoreType.REGULAR
    hbm, vmem = pl.BlockSpec(memory_space=pl.ANY), pl.BlockSpec(memory_space=pltpu.VMEM)
    return pl.pallas_call(
        functools.partial(kernel, top, slots),
        out_shape=jax.ShapeDtypeStruct((tokens, depth), BF16),
        in_specs=[hbm, vmem, vmem] + [hbm] * 6,
        out_specs=hbm,
        scratch_shapes=[
            pltpu.VMEM((8, padded, tokens), jnp.int32),
            pltpu.VMEM((8, padded, tokens), F32),
            pltpu.VMEM((8, rows, tokens), BF16),
            pltpu.VMEM((8, tokens, rows), BF16),
            pltpu.VMEM((2 * nq, 4, tokens, W), BF16),
            pltpu.VMEM((2 * own, 4 * slots, ff), F32),
            pltpu.VMEM((4 * NT, tokens, W), F32),
            pltpu.VMEM((own, 4 * slots, ff), BF16),
            pltpu.VMEM((2, tokens, ff), BF16),
            pltpu.VMEM((4, 2 * W, ff), BF16),
            pltpu.VMEM((4, ff, W), BF16),
            pltpu.VMEM((2, ff, W), BF16),
            pltpu.VMEM((own, 4, slots, 2 * W), BF16),
            pltpu.VMEM((4, own, slots, W), BF16),
            pltpu.VMEM((2, 4, tokens, W), BF16),
            pltpu.VMEM((2, 4, tokens, W), BF16),
            pltpu.VMEM((NL, 3, tokens, W), BF16),
            pltpu.VMEM((NL, 3, tokens, W), BF16),
            pltpu.VMEM((2, 3, tokens, W), BF16),
            pltpu.VMEM((2, 3, tokens, W), BF16),
            pltpu.VMEM((2, tokens, W), BF16),
            dma((8,)),
            dma((7,)),
            dma((8,)),
            dma((7,)),
            dma((2 * nq, 4)),
            dma((3, 4, 2)),
            dma((4,)),
            dma((4,)),
            dma((2,)),
            dma((2,)),
            dma((2,)),
            dma((NL, 4)),
            dma((NL, 4)),
            dma((2, 4)),
            dma((2, 4)),
            dma((2,)),
            regular((4,)),
            regular((4,)),
            regular,
        ],
        compiler_params=pltpu.CompilerParams(
            collective_id=0, has_side_effects=True, vmem_limit_bytes=67_043_328
        ),
    )(x, place, gate, wg, wu, wd, sg, su, sd)


def solution(mesh):
    members = mesh.shape["ep"]

    def local(x, expert, slot, gate, w_gate, w_up, w_down, s_gate, s_up, s_down):
        own, (tokens, top) = w_gate.shape[0], expert.shape[2:]
        experts = own * members
        slots = 5 * tokens * top // (4 * experts)
        place = jnp.where(slot[0, 0] < slots, expert[0, 0] * slots + slot[0, 0], -1).T
        weight = gate[0, 0].astype(BF16).astype(F32).T
        pad = ((0, -top % 8), (0, 0))
        place, weight = jnp.pad(place, pad, constant_values=-1), jnp.pad(weight, pad)
        y = moe(x[0, 0], place, weight, top, slots, w_gate, w_up, w_down, s_gate, s_up, s_down)
        return y[None, None]

    by_token = P("dp", "ep", None, None)
    by_expert = P("ep", None, None)
    whole = P(None, None)
    return jax.shard_map(
        local,
        mesh=mesh,
        in_specs=(by_token,) * 4 + (by_expert,) * 3 + (whole,) * 3,
        out_specs=by_token,
        check_vma=False,
    )
```
